16 devices in a mesh: rep: 2 (over y, z), dp: 8 (over x, core).
Axes of the slice: x: 4, y: 2, z: 1, core: 2. Of those that a mesh axis runs over, the one named last changes fastest.
The devices are a block of a 4x4x8 slice.
Arguments:
- g_w_gate: bfloat16 [16, 2, 1536, 4096], P(('rep', 'dp')), parts along dimension 0
- g_w_up: bfloat16 [16, 2, 1536, 4096], P(('rep', 'dp')), parts along dimension 0
- g_w_down: bfloat16 [16, 2, 4096, 1536], P(('rep', 'dp')), parts along dimension 0
- w_gate: bfloat16 [2, 1536, 4096], replicated
- w_up: bfloat16 [2, 1536, 4096], replicated
- w_down: bfloat16 [2, 4096, 1536], replicated
- m_w_gate: float32 [2, 1536, 4096], P(None, 'dp')
- m_w_up: float32 [2, 1536, 4096], P(None, 'dp')
- m_w_down: float32 [2, 4096, 1536], P(None, 'dp')
- v_w_gate: float32 [2, 1536, 4096], P(None, 'dp')
- v_w_up: float32 [2, 1536, 4096], P(None, 'dp')
- v_w_down: float32 [2, 4096, 1536], P(None, 'dp')
Outputs:
- output 1: bfloat16 [4, 1536, 4096], P('rep'), parts along dimension 0
- output 2: bfloat16 [4, 1536, 4096], P('rep'), parts along dimension 0
- output 3: bfloat16 [4, 4096, 1536], P('rep'), parts along dimension 0
- output 4: float32 [4, 1536, 4096], P('rep', 'dp'), parts along dimension 0
- output 5: float32 [4, 1536, 4096], P('rep', 'dp'), parts along dimension 0
- output 6: float32 [4, 4096, 1536], P('rep', 'dp'), parts along dimension 0
- output 7: float32 [4, 1536, 4096], P('rep', 'dp'), parts along dimension 0
- output 8: float32 [4, 1536, 4096], P('rep', 'dp'), parts along dimension 0
- output 9: float32 [4, 4096, 1536], P('rep', 'dp'), parts along dimension 0
There are 2 independent parts. The reference program is written for one: setup_inputs(seed, part) draws one part's arguments, and reference() takes and returns one part's arrays. A program takes and returns all parts, laid end to end along the dimension named above; an argument that names none is the same for every part.
All inputs are finite; a program needn't handle non-finite values.
Results may differ from the reference program's by a relative error of at most 0.022.
Values are sent between devices in bfloat16 or wider.
A program may use at most 768 MiB of HBM per device.

```python
import jax
import jax.numpy as jnp
from jax import lax

DEVICES = 8
D = 1536
FF = 4096
LAYERS = 2
NAMES = ("w_gate", "w_up", "w_down")
SHAPES = {"w_gate": (LAYERS, D, FF), "w_up": (LAYERS, D, FF), "w_down": (LAYERS, FF, D)}


def setup_inputs(seed: int = 0, part: int = 0) -> dict:
    kz, *keys = jax.random.split(jax.random.key(seed), 1 + 5 * len(NAMES))
    loud = 2.0 ** jax.random.uniform(kz, (), jnp.float32, -1.0, 1.0)
    drawn = {}
    for name, key, both in zip(NAMES, keys[:3], keys[3:6], strict=True):
        own = jax.random.normal(jax.random.fold_in(key, part), (DEVICES, *SHAPES[name]), jnp.float32)
        shared = jax.random.normal(jax.random.fold_in(both, part), SHAPES[name], jnp.float32)
        drawn["g_" + name] = (loud * (0.7 * shared / DEVICES + 0.7 * own * DEVICES**-0.5)).astype(jnp.bfloat16)
    for name, key in zip(NAMES, keys[6:9], strict=True):
        drawn[name] = (jax.random.normal(key, SHAPES[name], jnp.float32) * SHAPES[name][1] ** -0.5).astype(jnp.bfloat16)
    for name, key in zip(NAMES, keys[9:12], strict=True):
        drawn["m_" + name] = loud * 0.5 * jax.random.normal(key, SHAPES[name], jnp.float32)
    for name, key in zip(NAMES, keys[12:15], strict=True):
        drawn["v_" + name] = loud * loud * jax.random.uniform(key, SHAPES[name], jnp.float32, 0.5, 1.5)
    return drawn


def adamw(w, m, v, g):
    m = 0.9 * m + 0.1 * g
    v = 0.95 * v + 0.05 * g * g
    step = m * lax.rsqrt(v + 1e-8) + 0.1 * w
    return (w - 0.02 * step).astype(jnp.bfloat16), m, v


def reference(g_w_gate, g_w_up, g_w_down, w_gate, w_up, w_down, m_w_gate, m_w_up, m_w_down, v_w_gate, v_w_up, v_w_down):
    def total(terms):
        return lax.scan(lambda so_far, term: (so_far + term.astype(jnp.float32), None), jnp.zeros(terms.shape[1:], jnp.float32), terms)[0]

    gradients = [total(terms).astype(jnp.bfloat16).astype(jnp.float32) for terms in (g_w_gate, g_w_up, g_w_down)]
    new = [
        adamw(w.astype(jnp.float32), m, v, g)
        for w, m, v, g in zip((w_gate, w_up, w_down), (m_w_gate, m_w_up, m_w_down), (v_w_gate, v_w_up, v_w_down), gradients, strict=True)
    ]
    return tuple(one[which] for which in range(3) for one in new)
```

```python
import functools

import jax
import jax.numpy as jnp
from jax import lax
from jax.experimental import pallas as pl
from jax.experimental.pallas import tpu as pltpu
from jax.sharding import PartitionSpec as P

MESH = pl.DeviceIdType.MESH
F32, BF16 = jnp.float32, jnp.bfloat16
SPLIT = 2
GATHERED = 2
BATCH = 8
SLOTS = 5


def adamw(w, m, v, g):
    m = 0.9 * m + 0.1 * g
    v = 0.95 * v + 0.05 * g * g
    step = m * lax.rsqrt(v + 1e-8) + 0.1 * w
    return (w - 0.02 * step).astype(BF16), m, v


def tiles(x):
    *lead, rows, columns = x.shape
    x = x.reshape(*lead, rows // 8, 8, columns // 128, 128)
    return jnp.swapaxes(x, -3, -2).reshape(-1, 8, 128)


def untiles(x, shape):
    *lead, rows, columns = shape
    x = x.reshape(*lead, rows // 8, columns // 128, 8, 128)
    return jnp.swapaxes(x, -3, -2).reshape(shape)


def kernel(n, layers, *refs):
    weights = 3
    g, w, m, v = (refs[i * weights : (i + 1) * weights] for i in range(4))
    refs = refs[4 * weights :]
    gathered, block_out, sums = refs[:GATHERED], refs[GATHERED:weights], refs[weights : 2 * weights]
    (own, sib, s1, s2p, s2m, r1, r2p, r2m, mb, vb, wb, gb, new) = refs[2 * weights : 2 * weights + 13]
    (own_sem, sib_send, sib_recv, ring_send, ring_recv, mvw_sem, g_sem, ag_send, ag_recv, out_sem) = refs[2 * weights + 13 :]

    chips = n // 2
    me = lax.axis_index("dp")
    x, c = me // 2, me % 2
    right, left = (me + 2) % n, (me + n - 2) % n
    other = 2 * x + 1 - c
    opposite = (me + n // 2) % n
    block = g[0].shape[0] // layers // n
    layer = block * n
    size = block // SPLIT
    half = size // 2
    per_weight = layers * SPLIT
    chunks = weights * per_weight
    ag_chunks = GATHERED * per_weight

    barrier = pltpu.get_barrier_semaphore()
    for peer in (right, left, other):
        pl.semaphore_signal(barrier, inc=1, device_id={"dp": peer}, device_id_type=MESH)
    pl.semaphore_wait(barrier, 3)

    def place(k):
        unit, s = divmod(k, SPLIT)
        which, at = divmod(unit, layers)
        return which, at, s

    def at_whole(k, owner):
        _, at, s = place(k)
        return pl.ds(at * layer + owner * block + s * size, size)

    def at_block(k):
        _, at, s = place(k)
        return pl.ds(at * block + s * size, size)

    def first(ds):
        return pl.ds(ds.start, half)

    def last(ds):
        return pl.ds(ds.start + half, half)

    def remote(src, dst, send, recv, peer):
        return pltpu.make_async_remote_copy(
            src_ref=src, dst_ref=dst, send_sem=send, recv_sem=recv, device_id={"dp": peer}, device_id_type=MESH
        )

    def work(t):
        return [(k, js) for k, js in ((t + 1, (2,)), (t - 1, (1, 3)), (t - 3, (0,))) if 0 <= k < chunks]

    def own_copy(t, k, j):
        owner = (x + j) % chips * 2 + c
        return pltpu.make_async_copy(g[place(k)[0]].at[at_whole(k, owner)], own.at[t % 2, j], own_sem.at[t % 2, j])

    def sib_copy(t, k, j):
        owner = (x + j) % chips * 2 + 1 - c
        return remote(
            g[place(k)[0]].at[at_whole(k, owner)], sib.at[t % 4, j], sib_send.at[t % 2, j], sib_recv.at[t % 4, j], other
        )

    def mvw_copies(t, k):
        which = place(k)[0]
        return [
            pltpu.make_async_copy(m[which].at[at_block(k)], mb.at[t % 2], mvw_sem.at[t % 2, 0]),
            pltpu.make_async_copy(v[which].at[at_block(k)], vb.at[t % 2], mvw_sem.at[t % 2, 1]),
            pltpu.make_async_copy(w[which].at[at_whole(k, me)], wb.at[t % 2], mvw_sem.at[t % 2, 2]),
        ]

    def load(t):
        for k, js in work(t):
            for j in js:
                sib_copy(t, k, j).start()
                own_copy(t, k, j).start()
            if js == (0,):
                for copy in mvw_copies(t, k):
                    copy.start()

    def loaded(t, k, js):
        for j in js:
            own_copy(t, k, j).wait()
            sib_copy(t, k, j).wait()
        if js == (0,):
            for copy in mvw_copies(t, k):
                copy.wait()

    A, B = pl.ds(0, half), pl.ds(half, half)

    def ring1(t):
        return [
            remote(s1.at[t % 2, A], r1.at[t % SLOTS, A], ring_send.at[t % 2, 0], ring_recv.at[t % SLOTS, 0], right),
            remote(s1.at[t % 2, B], r1.at[t % SLOTS, B], ring_send.at[t % 2, 1], ring_recv.at[t % SLOTS, 1], left),
        ]

    def ring2(t):
        return [
            remote(s2p.at[t % 2], r2p.at[t % SLOTS], ring_send.at[t % 2, 2], ring_recv.at[t % SLOTS, 2], right),
            remote(s2m.at[t % 2], r2m.at[t % SLOTS], ring_send.at[t % 2, 3], ring_recv.at[t % SLOTS, 3], left),
        ]

    def rings(t):
        return (ring1(t) if 0 <= t < chunks else []) + (ring2(t) if 0 <= t - 2 < chunks else [])

    def each(count, body):
        def step(i, carry):
            body(pl.ds(pl.multiple_of(i * BATCH, BATCH), BATCH), i * BATCH)
            return carry

        lax.fori_loop(0, count // BATCH, step, 0)

    def pair(t, j, ds):
        return own[t % 2, j, ds].astype(F32) + sib[t % 4, j, ds].astype(F32)

    def stage1(t):
        def body(ds, _):
            s1[(t + 1) % 2, ds] = pair(t, 2, ds).astype(BF16)

        each(size, body)

    def stage2(t):
        def body(a, i):
            b = pl.ds(pl.multiple_of(half + i, BATCH), BATCH)
            s2p[(t + 1) % 2, a] = (pair(t, 1, a) + r1[(t - 1) % SLOTS, a].astype(F32)).astype(BF16)
            s2m[(t + 1) % 2, b] = (pair(t, 3, b) + r1[(t - 1) % SLOTS, b].astype(F32)).astype(BF16)
            s2p[(t + 1) % 2, b] = pair(t, 1, b).astype(BF16)
            s2m[(t + 1) % 2, a] = pair(t, 3, a).astype(BF16)

        each(half, body)

    def stage3(t, k):
        def body(ds, _):
            total = pair(t, 0, ds) + r2p[(t - 1) % SLOTS, ds].astype(F32) + r2m[(t - 1) % SLOTS, ds].astype(F32)
            total = total.astype(BF16)
            gb[t % 2, ds] = total
            new[k, ds] = adamw(wb[t % 2, ds].astype(F32), mb[t % 2, ds], vb[t % 2, ds], total.astype(F32))[0]

        each(size, body)

    def sum_out(t, k):
        return pltpu.make_async_copy(gb.at[t % 2], sums[place(k)[0]].at[at_block(k)], g_sem.at[t % 2])

    def block_copy(k):
        which = place(k)[0]
        return pltpu.make_async_copy(new.at[k], block_out[which - GATHERED].at[at_block(k)], out_sem.at[k])

    def local_copy(k):
        return pltpu.make_async_copy(new.at[k], gathered[place(k)[0]].at[at_whole(k, me)], out_sem.at[k])

    def spread(k, some=(0, 1, 2)):
        to = gathered[place(k)[0]].at[at_whole(k, me)]
        peers = right, left, other
        return [remote(new.at[k], to, ag_send.at[k, i], ag_recv.at[k, i], peers[i]) for i in some]

    def passed(k, i, owner, peer, part=None):
        ds = at_whole(k, owner)
        ref = gathered[place(k)[0]].at[part(ds) if part else ds]
        return remote(ref, ref, ag_send.at[k, i], ag_recv.at[k, i], peer)

    def forward(k):
        return [passed(k, 3, left, right, first), passed(k, 4, right, left, last)]

    def across(k):
        return [passed(k, 5, left, other), passed(k, 6, right, other)]

    def across_opposite(k):
        return [passed(k, 7, opposite, other)]

    ticks = range(-1, max(chunks + 3, ag_chunks + 8))
    load(-1)
    for t in ticks:
        for copy in rings(t - 1):
            copy.wait()
        k = t - 6
        if 0 <= k < ag_chunks:
            for copy in spread(k, (0, 1)):
                copy.wait_recv()
            for copy in forward(k) + across(k):
                copy.start()
        k = t - 8
        if 0 <= k < ag_chunks:
            for copy in forward(k):
                copy.wait_recv()
            for copy in across_opposite(k):
                copy.start()
        load(t + 1)
        for k, js in work(t):
            loaded(t, k, js)
            if js == (2,):
                stage1(t)
                for copy in ring1(t + 1):
                    copy.start()
            elif js == (1, 3):
                stage2(t)
                for copy in ring2(t + 1):
                    copy.start()
            else:
                if k >= 2:
                    sum_out(t - 2, k - 2).wait()
                stage3(t, k)
                sum_out(t, k).start()
                if k < ag_chunks:
                    for copy in spread(k):
                        copy.start()
                    local_copy(k).start()
                else:
                    block_copy(k).start()

    for k in range(max(chunks - 2, 0), chunks):
        sum_out(k + 3, k).wait()
    for k in range(ag_chunks, chunks):
        block_copy(k).wait()
    for k in range(ag_chunks):
        local_copy(k).wait()
        for copy in spread(k) + forward(k):
            copy.wait_send()
        spread(k, (2,))[0].wait_recv()
        for copy in across(k) + across_opposite(k):
            copy.wait()


def exchange(n, layers, terms, weights, m, v):
    everywhere = pl.BlockSpec(memory_space=pl.ANY)
    block = terms[0].shape[0] // layers // n
    size = block // SPLIT
    count = len(weights)
    chunks = count * layers * SPLIT
    ag_chunks = GATHERED * layers * SPLIT
    tile = (8, 128)
    buffer = lambda *lead, dtype=BF16: pltpu.VMEM((*lead, *tile), dtype)
    dma = pltpu.SemaphoreType.DMA
    out = pl.pallas_call(
        functools.partial(kernel, n, layers),
        out_shape=[jax.ShapeDtypeStruct(x.shape, BF16) for x in weights[:GATHERED]]
        + [jax.ShapeDtypeStruct(x.shape, BF16) for x in m[GATHERED:]]
        + [jax.ShapeDtypeStruct(x.shape, BF16) for x in m],
        in_specs=[everywhere] * (4 * count),
        out_specs=[everywhere] * (2 * count),
        scratch_shapes=[
            buffer(2, 4, size),
            buffer(4, 4, size),
            *[buffer(2, size)] * 3,
            *[buffer(SLOTS, size)] * 3,
            *[buffer(2, size, dtype=F32)] * 2,
            buffer(2, size),
            buffer(2, size),
            buffer(chunks, size),
            dma((2, 4)),
            dma((2, 4)),
            dma((4, 4)),
            dma((2, 4)),
            dma((SLOTS, 4)),
            dma((2, 3)),
            dma((2,)),
            dma((ag_chunks, 8)),
            dma((ag_chunks, 8)),
            dma((chunks,)),
        ],
        compiler_params=pltpu.CompilerParams(collective_id=0, has_side_effects=True, vmem_limit_bytes=62 * 2**20),
    )(*terms, *weights, *m, *v)
    return out[:GATHERED], out[GATHERED:count], out[count:]


def copy_kernel(x, *rest):
    rest[-1][...] = x[...]


def copied(x, whole=None, part=0, parts=1, into=None):
    steps = 8
    size = x.shape[0] // steps
    out = jax.ShapeDtypeStruct((x.shape[0] * parts, *x.shape[1:]), x.dtype)
    extra = [] if into is None else [into]
    return pl.pallas_call(
        copy_kernel,
        grid=(steps,),
        out_shape=out,
        in_specs=[pl.BlockSpec((size, 8, 128), lambda i: (i, 0, 0))] + [pl.BlockSpec(memory_space=pl.ANY)] * len(extra),
        out_specs=pl.BlockSpec((size, 8, 128), lambda i: (i + part * steps, 0, 0)),
        input_output_aliases={1: 0} if extra else {},
        cost_estimate=pl.CostEstimate(flops=0, bytes_accessed=2 * x.size * x.dtype.itemsize, transcendentals=0),
        compiler_params=pltpu.CompilerParams(vmem_limit_bytes=32 * 2**20),
    )(x, *extra)


def solution(mesh):
    n = mesh.shape["dp"]

    def step(*arrays):
        terms, weights, m, v = (arrays[i : i + 3] for i in (0, 3, 6, 9))
        layers = weights[0].shape[0]
        m_tiles, v_tiles = [tiles(a) for a in m], [tiles(a) for a in v]
        landed, blocks, sums = exchange(n, layers, [tiles(t[0]) for t in terms], [tiles(a) for a in weights], m_tiles, v_tiles)
        whole = []
        for one in blocks:
            parts = [lax.all_gather(p, "dp", axis=0, tiled=True) for p in jnp.split(one, layers)]
            result = None
            for i, part in enumerate(parts):
                result = copied(part, part=i, parts=layers, into=result)
            whole.append(result)
        whole = [copied(a) for a in landed] + whole
        new_m, new_v = [], []
        for mm, vv, s in zip(m_tiles, v_tiles, sums, strict=True):
            _, a, b = adamw(jnp.zeros((), F32), mm, vv, s.astype(F32))
            new_m.append(a)
            new_v.append(b)
        return (
            *(untiles(a, like.shape) for a, like in zip(whole, weights, strict=True)),
            *(untiles(a, like.shape) for a, like in zip(new_m, m, strict=True)),
            *(untiles(a, like.shape) for a, like in zip(new_v, v, strict=True)),
        )

    all_of, cut = P(None, None, None), P(None, "dp", None)
    return jax.shard_map(
        step,
        mesh=mesh,
        in_specs=(P(("rep", "dp"), None, None, None),) * 3 + (all_of,) * 3 + (cut,) * 6,
        out_specs=(P("rep", None, None),) * 3 + (P("rep", "dp", None),) * 6,
        check_vma=False,
    )
```

```python
import functools

import jax
import jax.numpy as jnp
from jax import lax
from jax.experimental import pallas as pl
from jax.experimental.pallas import tpu as pltpu
from jax.sharding import PartitionSpec as P


MESH = pl.DeviceIdType.MESH
F32, BF16 = jnp.float32, jnp.bfloat16
SPLIT = 2
BATCH = 8
SLOTS = 5


def adamw(w, m, v, g):
    m = 0.9 * m + 0.1 * g
    v = 0.95 * v + 0.05 * g * g
    step = m * lax.rsqrt(v + 1e-8) + 0.1 * w
    return (w - 0.02 * step).astype(BF16), m, v


def tiles(x):
    *lead, rows, columns = x.shape
    x = x.reshape(*lead, rows // 8, 8, columns // 128, 128)
    return jnp.swapaxes(x, -3, -2).reshape(-1, 8, 128)


def untiles(x, shape):
    *lead, rows, columns = shape
    x = x.reshape(*lead, rows // 8, columns // 128, 8, 128)
    return jnp.swapaxes(x, -3, -2).reshape(shape)


def kernel(n, layers, *refs):
    weights = 3
    g, w, m, v = (refs[i * weights : (i + 1) * weights] for i in range(4))
    refs = refs[4 * weights :]
    landed, go_right, go_left, sums = (refs[i * weights : (i + 1) * weights] for i in range(4))
    refs = refs[2 * weights :]
    (own, sib, s1, s2p, s2m, r1, r2p, r2m, mb, vb, wb, gb, new) = refs[2 * weights : 2 * weights + 13]
    (own_sem, sib_send, sib_recv, ring_send, ring_recv, mvw_sem, g_sem, ag_send, ag_recv, out_sem) = refs[2 * weights + 13 :]

    chips = n // 2
    me = lax.axis_index("dp")
    x, c = me // 2, me % 2
    right, left = (me + 2) % n, (me + n - 2) % n
    other = 2 * x + 1 - c
    block = g[0].shape[0] // layers // n
    layer = block * n
    size = block // SPLIT
    half = size // 2
    per_weight = layers * SPLIT
    chunks = weights * per_weight

    barrier = pltpu.get_barrier_semaphore()
    for peer in (right, left, other):
        pl.semaphore_signal(barrier, inc=1, device_id={"dp": peer}, device_id_type=MESH)
    pl.semaphore_wait(barrier, 3)

    def place(k):
        unit, s = divmod(k, SPLIT)
        which, at = divmod(unit, layers)
        return which, at, s

    def at_whole(k, owner):
        _, at, s = place(k)
        return pl.ds(at * layer + owner * block + s * size, size)

    def at_block(k):
        _, at, s = place(k)
        return pl.ds(at * block + s * size, size)

    def first(ds):
        return pl.ds(ds.start, half)

    def last(ds):
        return pl.ds(ds.start + half, half)

    def remote(src, dst, send, recv, peer):
        return pltpu.make_async_remote_copy(
            src_ref=src, dst_ref=dst, send_sem=send, recv_sem=recv, device_id={"dp": peer}, device_id_type=MESH
        )

    def work(t):
        return [(k, js) for k, js in ((t + 1, (2,)), (t - 1, (1, 3)), (t - 3, (0,))) if 0 <= k < chunks]

    def own_copy(t, k, j):
        owner = (x + j) % chips * 2 + c
        return pltpu.make_async_copy(g[place(k)[0]].at[at_whole(k, owner)], own.at[t % 2, j], own_sem.at[t % 2, j])

    def sib_copy(t, k, j):
        owner = (x + j) % chips * 2 + 1 - c
        return remote(
            g[place(k)[0]].at[at_whole(k, owner)], sib.at[t % 4, j], sib_send.at[t % 2, j], sib_recv.at[t % 4, j], other
        )

    def mvw_copies(t, k):
        which = place(k)[0]
        return [
            pltpu.make_async_copy(m[which].at[at_block(k)], mb.at[t % 2], mvw_sem.at[t % 2, 0]),
            pltpu.make_async_copy(v[which].at[at_block(k)], vb.at[t % 2], mvw_sem.at[t % 2, 1]),
            pltpu.make_async_copy(w[which].at[at_whole(k, me)], wb.at[t % 2], mvw_sem.at[t % 2, 2]),
        ]

    def load(t):
        for k, js in work(t):
            for j in js:
                sib_copy(t, k, j).start()
                own_copy(t, k, j).start()
            if js == (0,):
                for copy in mvw_copies(t, k):
                    copy.start()

    def loaded(t, k, js):
        for j in js:
            own_copy(t, k, j).wait()
            sib_copy(t, k, j).wait()
        if js == (0,):
            for copy in mvw_copies(t, k):
                copy.wait()

    A, B = pl.ds(0, half), pl.ds(half, half)

    def ring1(t):
        return [
            remote(s1.at[t % 2, A], r1.at[t % SLOTS, A], ring_send.at[t % 2, 0], ring_recv.at[t % SLOTS, 0], right),
            remote(s1.at[t % 2, B], r1.at[t % SLOTS, B], ring_send.at[t % 2, 1], ring_recv.at[t % SLOTS, 1], left),
        ]

    def ring2(t):
        return [
            remote(s2p.at[t % 2], r2p.at[t % SLOTS], ring_send.at[t % 2, 2], ring_recv.at[t % SLOTS, 2], right),
            remote(s2m.at[t % 2], r2m.at[t % SLOTS], ring_send.at[t % 2, 3], ring_recv.at[t % SLOTS, 3], left),
        ]

    def rings(t):
        return (ring1(t) if 0 <= t < chunks else []) + (ring2(t) if 0 <= t - 2 < chunks else [])

    def each(count, body):
        def step(i, carry):
            body(pl.ds(pl.multiple_of(i * BATCH, BATCH), BATCH), i * BATCH)
            return carry

        lax.fori_loop(0, count // BATCH, step, 0)

    def pair(t, j, ds):
        return own[t % 2, j, ds].astype(F32) + sib[t % 4, j, ds].astype(F32)

    def stage1(t):
        def body(ds, _):
            s1[(t + 1) % 2, ds] = pair(t, 2, ds).astype(BF16)

        each(size, body)

    def stage2(t):
        def body(a, i):
            b = pl.ds(pl.multiple_of(half + i, BATCH), BATCH)
            s2p[(t + 1) % 2, a] = (pair(t, 1, a) + r1[(t - 1) % SLOTS, a].astype(F32)).astype(BF16)
            s2m[(t + 1) % 2, b] = (pair(t, 3, b) + r1[(t - 1) % SLOTS, b].astype(F32)).astype(BF16)
            s2p[(t + 1) % 2, b] = pair(t, 1, b).astype(BF16)
            s2m[(t + 1) % 2, a] = pair(t, 3, a).astype(BF16)

        each(half, body)

    def stage3(t, k):
        def body(ds, _):
            total = pair(t, 0, ds) + r2p[(t - 1) % SLOTS, ds].astype(F32) + r2m[(t - 1) % SLOTS, ds].astype(F32)
            total = total.astype(BF16)
            gb[t % 2, ds] = total
            new[k, ds] = adamw(wb[t % 2, ds].astype(F32), mb[t % 2, ds], vb[t % 2, ds], total.astype(F32))[0]

        each(size, body)

    def sum_out(t, k):
        return pltpu.make_async_copy(gb.at[t % 2], sums[place(k)[0]].at[at_block(k)], g_sem.at[t % 2])

    def local_copy(k):
        return pltpu.make_async_copy(new.at[k], landed[place(k)[0]].at[at_whole(k, me)], out_sem.at[k])

    def compact(k):
        _, at, s = place(k)
        return pl.ds(at * (block // 2) + s * half, half)

    def to_peer(k, i, src, dst, peer):
        return remote(src, dst, ag_send.at[k, i], ag_recv.at[k, i], peer)

    def spread(k, some=(0, 1, 2, 3, 4)):
        which, ds = place(k)[0], at_whole(k, me)
        front, back = landed[which].at[first(ds)], landed[which].at[last(ds)]
        plan = (
            (new.at[k, A], go_right[which].at[compact(k)], right),
            (new.at[k, B], go_left[which].at[compact(k)], left),
            (new.at[k, B], back, right),
            (new.at[k, A], front, left),
            (new.at[k], landed[which].at[ds], other),
        )
        return [to_peer(k, i, *plan[i]) for i in some]

    def across(k):
        which = place(k)[0]
        from_left, from_right = at_whole(k, left), at_whole(k, right)
        at = landed[which].at
        return [
            to_peer(k, 5, go_right[which].at[compact(k)], at[first(from_left)], other),
            to_peer(k, 6, go_left[which].at[compact(k)], at[last(from_right)], other),
            to_peer(k, 7, at[last(from_left)], at[last(from_left)], other),
            to_peer(k, 8, at[first(from_right)], at[first(from_right)], other),
        ]

    load(-1)
    for t in range(-1, chunks + 6):
        for copy in rings(t - 1):
            copy.wait()
        k = t - 6
        if 0 <= k < chunks:
            for copy in spread(k, (0, 1, 2, 3)):
                copy.wait_recv()
            for copy in across(k):
                copy.start()
        load(t + 1)
        for k, js in work(t):
            loaded(t, k, js)
            if js == (2,):
                stage1(t)
                for copy in ring1(t + 1):
                    copy.start()
            elif js == (1, 3):
                stage2(t)
                for copy in ring2(t + 1):
                    copy.start()
            else:
                if k >= 2:
                    sum_out(t - 2, k - 2).wait()
                stage3(t, k)
                for copy in spread(k):
                    copy.start()
                sum_out(t, k).start()
                local_copy(k).start()

    for k in range(max(chunks - 2, 0), chunks):
        sum_out(k + 3, k).wait()
    for k in range(chunks):
        local_copy(k).wait()
        for copy in spread(k):
            copy.wait_send()
        spread(k, (4,))[0].wait_recv()
        for copy in across(k):
            copy.wait()


def exchange(n, layers, terms, weights, m, v):
    everywhere = pl.BlockSpec(memory_space=pl.ANY)
    block = terms[0].shape[0] // layers // n
    size = block // SPLIT
    count = len(weights)
    chunks = count * layers * SPLIT
    tile = (8, 128)
    buffer = lambda *lead, dtype=BF16: pltpu.VMEM((*lead, *tile), dtype)
    array = lambda rows: jax.ShapeDtypeStruct((rows, *tile), BF16)
    dma = pltpu.SemaphoreType.DMA
    out = pl.pallas_call(
        functools.partial(kernel, n, layers),
        out_shape=[array(x.shape[0]) for x in weights]
        + [array(x.shape[0] // 2) for x in m * 2]
        + [array(x.shape[0]) for x in m],
        in_specs=[everywhere] * (4 * count),
        out_specs=[everywhere] * (4 * count),
        scratch_shapes=[
            buffer(2, 4, size),
            buffer(4, 4, size),
            *[buffer(2, size)] * 3,
            *[buffer(SLOTS, size)] * 3,
            *[buffer(2, size, dtype=F32)] * 2,
            buffer(2, size),
            buffer(2, size),
            buffer(chunks, size),
            dma((2, 4)),
            dma((2, 4)),
            dma((4, 4)),
            dma((2, 4)),
            dma((SLOTS, 4)),
            dma((2, 3)),
            dma((2,)),
            dma((chunks, 9)),
            dma((chunks, 9)),
            dma((chunks,)),
        ],
        compiler_params=pltpu.CompilerParams(collective_id=0, has_side_effects=True, vmem_limit_bytes=62 * 2**20),
    )(*terms, *weights, *m, *v)
    return (out[i * count : (i + 1) * count] for i in range(4))


def put(items, buffer, sems, out):
    into, outof, at = [], [], 0
    for i, (src, to) in enumerate(items):
        via = buffer.at[pl.ds(at, src.shape[0])]
        into.append(pltpu.make_async_copy(src, via, sems.at[0, i]))
        outof.append(pltpu.make_async_copy(via, out.at[pl.ds(to, src.shape[0])], sems.at[1, i]))
        at += src.shape[0]
    for copy in into:
        copy.start()
    for arrival, copy in zip(into, outof, strict=True):
        arrival.wait()
        copy.start()
    for copy in outof:
        copy.wait()


def near_kernel(n, layers, landed, go_right, go_left, out, buffer, sems):
    me = lax.axis_index("dp")
    other = me + 1 - 2 * (me % 2)
    block = landed.shape[0] // layers // n
    half = block // SPLIT // 2
    items = []
    for layer in range(layers):
        base = layer * n * block
        for owner in (me, other, (other + 2) % n, (other + n - 2) % n):
            at = base + owner * block
            items.append((landed.at[pl.ds(at, block)], at))
        for s in range(SPLIT):
            right, left = (base + owner % n * block + 2 * s * half for owner in (me + 2, me + n - 2))
            compact = pl.ds((layer * SPLIT + s) * half, half)
            items += [
                (landed.at[pl.ds(right, half)], right),
                (go_left.at[compact], right + half),
                (go_right.at[compact], left),
                (landed.at[pl.ds(left + half, half)], left + half),
            ]
    put(items, buffer, sems, out)


def far_kernel(n, layers, front, back, other_front, other_back, _, out, buffer, sems):
    me = lax.axis_index("dp")
    other = me + 1 - 2 * (me % 2)
    block = out.shape[0] // layers // n
    half = block // SPLIT // 2
    items = []
    for layer in range(layers):
        for s in range(SPLIT):
            compact = pl.ds((layer * SPLIT + s) * half, half)
            for owner, x, y in ((me, front, back), (other, other_front, other_back)):
                at = (layer * n + (owner + n // 2) % n) * block + 2 * s * half
                items += [(x.at[compact], at), (y.at[compact], at + half)]
    put(items, buffer, sems, out)


def placed(body, n, layers, count, share, like, operands, into=None):
    everywhere = pl.BlockSpec(memory_space=pl.ANY)
    operands = [*operands, *([] if into is None else [into])]
    return pl.pallas_call(
        functools.partial(body, n, layers),
        out_shape=jax.ShapeDtypeStruct(like.shape, like.dtype),
        in_specs=[everywhere] * len(operands),
        out_specs=everywhere,
        scratch_shapes=[pltpu.VMEM((int(share * like.shape[0]), 8, 128), BF16), pltpu.SemaphoreType.DMA((2, count))],
        input_output_aliases={} if into is None else {len(operands) - 1: 0},
        cost_estimate=pl.CostEstimate(flops=0, bytes_accessed=int(2 * share * like.size * like.dtype.itemsize), transcendentals=0),
        compiler_params=pltpu.CompilerParams(vmem_limit_bytes=67043328),
    )(*operands)


def solution(mesh):
    n = mesh.shape["dp"]
    to_right = [(i, (i + 2) % n) for i in range(n)]
    to_left = [(i, (i - 2) % n) for i in range(n)]
    to_other = [(i, i ^ 1) for i in range(n)]

    def step(*arrays):
        terms, weights, m, v = (arrays[i : i + 3] for i in (0, 3, 6, 9))
        layers = weights[0].shape[0]
        m_tiles, v_tiles, w_tiles = ([tiles(a) for a in group] for group in (m, v, weights))
        landed, go_right, go_left, sums = exchange(n, layers, [tiles(t[0]) for t in terms], w_tiles, m_tiles, v_tiles)
        passed = []
        for r, l in zip(go_right, go_left, strict=True):
            front = lax.ppermute(r, "dp", to_right)
            back = lax.ppermute(l, "dp", to_left)
            passed.append((front, back))
        new_m, new_v = [], []
        for mm, vv, s in zip(m_tiles, v_tiles, sums, strict=True):
            _, a, b = adamw(jnp.zeros((), F32), mm, vv, s.astype(F32))
            new_m.append(a)
            new_v.append(b)
        near = []
        for like, *x in zip(w_tiles, landed, go_right, go_left, strict=True):
            near.append(placed(near_kernel, n, layers, 4 * layers * (1 + SPLIT), 0.75, like, x))
        whole = []
        for like, out, pair in zip(w_tiles, near, passed, strict=True):
            pair = [*pair, *(lax.ppermute(a, "dp", to_other) for a in pair)]
            whole.append(placed(far_kernel, n, layers, 4 * layers * SPLIT, 0.25, like, pair, out))
        return (
            *(untiles(a, like.shape) for a, like in zip(whole, weights, strict=True)),
            *(untiles(a, like.shape) for a, like in zip(new_m, m, strict=True)),
            *(untiles(a, like.shape) for a, like in zip(new_v, v, strict=True)),
        )

    all_of, cut = P(None, None, None), P(None, "dp", None)
    return jax.shard_map(
        step,
        mesh=mesh,
        in_specs=(P(("rep", "dp"), None, None, None),) * 3 + (all_of,) * 3 + (cut,) * 6,
        out_specs=(P("rep", None, None),) * 3 + (P("rep", "dp", None),) * 6,
        check_vma=False,
    )
```

```python
import functools

import jax
import jax.numpy as jnp
from jax import lax
from jax.experimental import pallas as pl
from jax.experimental.pallas import tpu as pltpu
from jax.sharding import PartitionSpec as P


MESH = pl.DeviceIdType.MESH
F32, BF16 = jnp.float32, jnp.bfloat16
WEIGHTS = 3
GROUPS = WEIGHTS + 2
BATCH = 8
SLOTS = 5


def adamw(w, m, v, g):
    m = 0.9 * m + 0.1 * g
    v = 0.95 * v + 0.05 * g * g
    step = m * lax.rsqrt(v + 1e-8) + 0.1 * w
    return (w - 0.02 * step).astype(BF16), m, v


def tiles(x):
    *lead, rows, columns = x.shape
    x = x.reshape(*lead, rows // 8, 8, columns // 128, 128)
    return jnp.swapaxes(x, -3, -2).reshape(-1, 8, 128)


def untiles(x, shape):
    *lead, rows, columns = shape
    x = x.reshape(*lead, rows // 8, columns // 128, 8, 128)
    return jnp.swapaxes(x, -3, -2).reshape(shape)


def cuts(block, units):
    table = []
    for unit in range(units):
        start = 0
        for eighths in (1, 3, 4) if unit == 0 else (4, 3, 1) if unit == units - 1 else (4, 4):
            table.append((unit, start, block * eighths // 8))
            start += table[-1][2]
    return table


def groups_of(table, layers):
    units = table[-1][0] + 1
    owner = [min(unit // layers, WEIGHTS - 1) + (unit == units - 1) + (unit == units - 1 and start > 0) for unit, start, _ in table]
    return [[k for k, i in enumerate(owner) if i == j] for j in range(GROUPS)]


def halves(table, group):
    at, found = 0, []
    for k in group:
        unit, start, size = table[k]
        found.append((unit, start, size // 2, at))
        at += size // 2
    return found


def kernel(n, layers, *refs):
    weights = WEIGHTS
    g, w, m, v = (refs[i * weights : (i + 1) * weights] for i in range(4))
    refs = refs[4 * weights :]
    landed, sums = refs[:weights], refs[weights : 2 * weights]
    refs = refs[2 * weights :]
    go_right, go_left, refs = refs[:GROUPS], refs[GROUPS : 2 * GROUPS], refs[2 * GROUPS :]
    (own, sib, s1, s2p, s2m, r1, r2p, r2m, mb, vb, wb, gb, new) = refs[:13]
    (own_sem, sib_send, sib_recv, ring_send, ring_recv, mvw_sem, g_sem, ag_send, ag_recv, out_sem) = refs[13:]

    chips = n // 2
    me = lax.axis_index("dp")
    x, c = me // 2, me % 2
    right, left = (me + 2) % n, (me + n - 2) % n
    other = 2 * x + 1 - c
    block = g[0].shape[0] // layers // n
    layer = block * n
    table = cuts(block, weights * layers)
    groups = groups_of(table, layers)
    chunks = len(table)

    barrier = pltpu.get_barrier_semaphore()
    for peer in (right, left, other):
        pl.semaphore_signal(barrier, inc=1, device_id={"dp": peer}, device_id_type=MESH)
    pl.semaphore_wait(barrier, 3)

    def weight(k):
        return table[k][0] // layers

    def size(k):
        return table[k][2]

    def at_whole(k, owner):
        unit, start, count = table[k]
        return pl.ds(unit % layers * layer + owner * block + start, count)

    def at_block(k):
        unit, start, count = table[k]
        return pl.ds(unit % layers * block + start, count)

    def first(ds):
        return pl.ds(ds.start, ds.size // 2)

    def last(ds):
        return pl.ds(ds.start + ds.size // 2, ds.size // 2)

    def part(k):
        return pl.ds(0, size(k))

    def remote(src, dst, send, recv, peer):
        return pltpu.make_async_remote_copy(
            src_ref=src, dst_ref=dst, send_sem=send, recv_sem=recv, device_id={"dp": peer}, device_id_type=MESH
        )

    def work(t):
        return [(k, js) for k, js in ((t + 1, (2,)), (t - 1, (1, 3)), (t - 3, (0,))) if 0 <= k < chunks]

    def own_copy(t, k, j):
        owner = (x + j) % chips * 2 + c
        return pltpu.make_async_copy(g[weight(k)].at[at_whole(k, owner)], own.at[t % 2, j, part(k)], own_sem.at[t % 2, j])

    def sib_copy(t, k, j):
        owner = (x + j) % chips * 2 + 1 - c
        return remote(
            g[weight(k)].at[at_whole(k, owner)],
            sib.at[t % 4, j, part(k)],
            sib_send.at[t % 2, j],
            sib_recv.at[t % 4, j],
            other,
        )

    def mvw_copies(t, k):
        which = weight(k)
        return [
            pltpu.make_async_copy(m[which].at[at_block(k)], mb.at[t % 2, part(k)], mvw_sem.at[t % 2, 0]),
            pltpu.make_async_copy(v[which].at[at_block(k)], vb.at[t % 2, part(k)], mvw_sem.at[t % 2, 1]),
            pltpu.make_async_copy(w[which].at[at_whole(k, me)], wb.at[t % 2, part(k)], mvw_sem.at[t % 2, 2]),
        ]

    def load(t):
        for k, js in work(t):
            for j in js:
                sib_copy(t, k, j).start()
                own_copy(t, k, j).start()
            if js == (0,):
                for copy in mvw_copies(t, k):
                    copy.start()

    def loaded(t, k, js):
        for j in js:
            own_copy(t, k, j).wait()
            sib_copy(t, k, j).wait()
        if js == (0,):
            for copy in mvw_copies(t, k):
                copy.wait()

    def ring1(t):
        a, b = first(part(t)), last(part(t))
        return [
            remote(s1.at[t % 2, a], r1.at[t % SLOTS, a], ring_send.at[t % 2, 0], ring_recv.at[t % SLOTS, 0], right),
            remote(s1.at[t % 2, b], r1.at[t % SLOTS, b], ring_send.at[t % 2, 1], ring_recv.at[t % SLOTS, 1], left),
        ]

    def ring2(t):
        a = part(t - 2)
        return [
            remote(s2p.at[t % 2, a], r2p.at[t % SLOTS, a], ring_send.at[t % 2, 2], ring_recv.at[t % SLOTS, 2], right),
            remote(s2m.at[t % 2, a], r2m.at[t % SLOTS, a], ring_send.at[t % 2, 3], ring_recv.at[t % SLOTS, 3], left),
        ]

    def rings(t):
        return (ring1(t) if 0 <= t < chunks else []) + (ring2(t) if 0 <= t - 2 < chunks else [])

    def each(count, body):
        def step(i, carry):
            body(pl.ds(pl.multiple_of(i * BATCH, BATCH), BATCH), i * BATCH)
            return carry

        lax.fori_loop(0, count // BATCH, step, 0)

    def pair(t, j, ds):
        return own[t % 2, j, ds].astype(F32) + sib[t % 4, j, ds].astype(F32)

    def stage1(t, k):
        def body(ds, _):
            s1[(t + 1) % 2, ds] = pair(t, 2, ds).astype(BF16)

        each(size(k), body)

    def stage2(t, k):
        half = size(k) // 2

        def body(a, i):
            b = pl.ds(pl.multiple_of(half + i, BATCH), BATCH)
            s2p[(t + 1) % 2, a] = (pair(t, 1, a) + r1[(t - 1) % SLOTS, a].astype(F32)).astype(BF16)
            s2m[(t + 1) % 2, b] = (pair(t, 3, b) + r1[(t - 1) % SLOTS, b].astype(F32)).astype(BF16)
            s2p[(t + 1) % 2, b] = pair(t, 1, b).astype(BF16)
            s2m[(t + 1) % 2, a] = pair(t, 3, a).astype(BF16)

        each(half, body)

    def fresh(k):
        unit, start, count = table[k]
        return new.at[pl.ds(unit * block + start, count)]

    def stage3(t, k):
        at = fresh(k)

        def body(ds, _):
            total = pair(t, 0, ds) + r2p[(t - 1) % SLOTS, ds].astype(F32) + r2m[(t - 1) % SLOTS, ds].astype(F32)
            total = total.astype(BF16)
            gb[t % 2, ds] = total
            at[ds] = adamw(wb[t % 2, ds].astype(F32), mb[t % 2, ds], vb[t % 2, ds], total.astype(F32))[0]

        each(size(k), body)

    def sum_out(t, k):
        return pltpu.make_async_copy(gb.at[t % 2, part(k)], sums[weight(k)].at[at_block(k)], g_sem.at[t % 2])

    def local_copy(k):
        return pltpu.make_async_copy(fresh(k), landed[weight(k)].at[at_whole(k, me)], out_sem.at[k])

    def passing(refs, k):
        i, group = next((i, group) for i, group in enumerate(groups) if k in group)
        _, _, half, at = halves(table, group)[group.index(k)]
        return refs[i].at[pl.ds(at, half)]

    def to_peer(k, i, src, dst, peer):
        return remote(src, dst, ag_send.at[k, i], ag_recv.at[k, i], peer)

    def spread(k, some=(0, 1, 2, 3, 4)):
        at, mine, a, b = landed[weight(k)].at, at_whole(k, me), first(part(k)), last(part(k))
        plan = (
            (fresh(k).at[a], passing(go_right, k), right),
            (fresh(k).at[b], passing(go_left, k), left),
            (fresh(k).at[b], at[last(mine)], right),
            (fresh(k).at[a], at[first(mine)], left),
            (fresh(k), at[mine], other),
        )
        return [to_peer(k, i, *plan[i]) for i in some]

    def across(k, some=(0, 1, 2, 3)):
        at, from_left, from_right = landed[weight(k)].at, at_whole(k, left), at_whole(k, right)
        plan = (
            (passing(go_right, k), at[first(from_left)]),
            (passing(go_left, k), at[last(from_right)]),
            (at[last(from_left)], at[last(from_left)]),
            (at[first(from_right)], at[first(from_right)]),
        )
        return [to_peer(k, 5 + i, *plan[i], other) for i in some]

    load(-1)
    for t in range(-1, chunks + 6):
        for copy in rings(t - 1):
            copy.wait()
        k = t - 6
        if 0 <= k < chunks:
            for i in range(4):
                spread(k, (i,))[0].wait_recv()
                across(k, (i,))[0].start()
        load(t + 1)
        for k, js in work(t):
            loaded(t, k, js)
            if js == (2,):
                stage1(t, k)
                for copy in ring1(t + 1):
                    copy.start()
            elif js == (1, 3):
                stage2(t, k)
                for copy in ring2(t + 1):
                    copy.start()
            else:
                if k >= 2:
                    sum_out(t - 2, k - 2).wait()
                stage3(t, k)
                for copy in spread(k):
                    copy.start()
                sum_out(t, k).start()
                local_copy(k).start()

    for k in range(max(chunks - 2, 0), chunks):
        sum_out(k + 3, k).wait()
    for k in range(chunks):
        local_copy(k).wait()
        for copy in spread(k):
            copy.wait_send()
        spread(k, (4,))[0].wait_recv()
        for copy in across(k):
            copy.wait()


def exchange(n, layers, terms, weights, m, v):
    everywhere = pl.BlockSpec(memory_space=pl.ANY)
    block = terms[0].shape[0] // layers // n
    count = len(weights)
    table = cuts(block, count * layers)
    groups = groups_of(table, layers)
    chunks, size = len(table), max(entry[2] for entry in table)
    tile = (8, 128)
    buffer = lambda *lead, dtype=BF16: pltpu.VMEM((*lead, *tile), dtype)
    array = lambda rows: jax.ShapeDtypeStruct((rows, *tile), BF16)
    dma = pltpu.SemaphoreType.DMA
    shapes = [
        *[array(x.shape[0]) for x in (*weights, *m)],
        *[array(sum(table[k][2] for k in group) // 2) for group in groups * 2],
    ]
    out = pl.pallas_call(
        functools.partial(kernel, n, layers),
        out_shape=shapes,
        in_specs=[everywhere] * (4 * count),
        out_specs=[everywhere] * len(shapes),
        scratch_shapes=[
            buffer(2, 4, size),
            buffer(4, 4, size),
            *[buffer(2, size)] * 3,
            *[buffer(SLOTS, size)] * 3,
            *[buffer(2, size, dtype=F32)] * 2,
            buffer(2, size),
            buffer(2, size),
            buffer(count * layers * block),
            dma((2, 4)),
            dma((2, 4)),
            dma((4, 4)),
            dma((2, 4)),
            dma((SLOTS, 4)),
            dma((2, 3)),
            dma((2,)),
            dma((chunks, 9)),
            dma((chunks, 9)),
            dma((chunks,)),
        ],
        compiler_params=pltpu.CompilerParams(collective_id=0, has_side_effects=True, vmem_limit_bytes=62 * 2**20),
    )(*terms, *weights, *m, *v)
    passing = out[2 * count :]
    return out[:count], passing[:GROUPS], passing[GROUPS:], out[count : 2 * count]


def put(items, buffer, sems):
    into, outof, at = [], [], 0
    for i, (src, dst) in enumerate(items):
        via = buffer.at[pl.ds(at, src.shape[0])]
        into.append(pltpu.make_async_copy(src, via, sems.at[0, i]))
        outof.append(pltpu.make_async_copy(via, dst, sems.at[1, i]))
        at += src.shape[0]
    for copy in into:
        copy.start()
    for arrival, copy in zip(into, outof, strict=True):
        arrival.wait()
        copy.start()
    for copy in outof:
        copy.wait()


def near_kernel(n, layers, table, groups, *refs):
    landed, refs = refs[:WEIGHTS], refs[WEIGHTS:]
    go_right, go_left, refs = refs[:GROUPS], refs[GROUPS : 2 * GROUPS], refs[2 * GROUPS :]
    out, (buffer, sems) = refs[:WEIGHTS], refs[WEIGHTS:]
    me = lax.axis_index("dp")
    other = me + 1 - 2 * (me % 2)
    right, left = (me + 2) % n, (me + n - 2) % n
    block = landed[0].shape[0] // layers // n
    items = []

    def same(unit, owner, start, count):
        ds = pl.ds((unit % layers * n + owner) * block + start, count)
        items.append((landed[unit // layers].at[ds], out[unit // layers].at[ds]))

    def passing(ref, at, unit, owner, start, count):
        ds = pl.ds((unit % layers * n + owner) * block + start, count)
        items.append((ref.at[pl.ds(at, count)], out[unit // layers].at[ds]))

    for unit in range(WEIGHTS * layers):
        for owner in (me, other, (other + 2) % n, (other + n - 2) % n):
            same(unit, owner, 0, block)
        for i, group in enumerate(groups):
            for at_unit, start, half, at in halves(table, group):
                if at_unit == unit:
                    same(unit, right, start, half)
                    passing(go_left[i], at, unit, right, start + half, half)
                    passing(go_right[i], at, unit, left, start, half)
                    same(unit, left, start + half, half)
    put(items, buffer, sems)


def far_kernel(n, layers, pieces, front, back, other_front, other_back, _, out, buffer, sems):
    me = lax.axis_index("dp")
    other = me + 1 - 2 * (me % 2)
    block = out.shape[0] // layers // n
    items = []
    for unit, start, half, at in pieces:
        for owner, x, y in ((me, front, back), (other, other_front, other_back)):
            to = (unit % layers * n + (owner + n // 2) % n) * block + start
            items += [(x.at[pl.ds(at, half)], out.at[pl.ds(to, half)]), (y.at[pl.ds(at, half)], out.at[pl.ds(to + half, half)])]
    put(items, buffer, sems)


def placed(body, count, amount, shapes, operands, into=None):
    everywhere = pl.BlockSpec(memory_space=pl.ANY)
    operands = [*operands, *([] if into is None else [into])]
    return pl.pallas_call(
        body,
        out_shape=[jax.ShapeDtypeStruct(x.shape, x.dtype) for x in shapes],
        in_specs=[everywhere] * len(operands),
        out_specs=[everywhere] * len(shapes),
        scratch_shapes=[pltpu.VMEM((amount, 8, 128), BF16), pltpu.SemaphoreType.DMA((2, count))],
        input_output_aliases={} if into is None else {len(operands) - 1: 0},
        cost_estimate=pl.CostEstimate(flops=0, bytes_accessed=2 * amount * 1024 * 2, transcendentals=0),
        compiler_params=pltpu.CompilerParams(vmem_limit_bytes=67043328),
    )(*operands)


def solution(mesh):
    n = mesh.shape["dp"]
    to_right = [(i, (i + 2) % n) for i in range(n)]
    to_left = [(i, (i - 2) % n) for i in range(n)]
    to_other = [(i, i ^ 1) for i in range(n)]

    def step(*arrays):
        terms, weights, m, v = (arrays[i : i + 3] for i in (0, 3, 6, 9))
        layers = weights[0].shape[0]
        m_tiles, v_tiles, w_tiles = ([tiles(a) for a in group] for group in (m, v, weights))
        landed, go_right, go_left, sums = exchange(n, layers, [tiles(t[0]) for t in terms], w_tiles, m_tiles, v_tiles)
        passed = []
        for i, (r, l) in enumerate(zip(go_right, go_left, strict=True)):
            front = lax.ppermute(r, "dp", to_right)
            back = lax.ppermute(l, "dp", to_left)
            passed.append((front, back))
        new_m, new_v = [], []
        for mm, vv, s in zip(m_tiles, v_tiles, sums, strict=True):
            _, a, b = adamw(jnp.zeros((), F32), mm, vv, s.astype(F32))
            new_m.append(a)
            new_v.append(b)
        block = m_tiles[0].shape[0] // layers
        table = cuts(block, WEIGHTS * layers)
        groups = groups_of(table, layers)
        body = functools.partial(near_kernel, n, layers, table, groups)
        count, amount = 4 * (WEIGHTS * layers + len(table)), (n - 2) * WEIGHTS * layers * block
        whole = [*placed(body, count, amount, w_tiles, [*landed, *go_right, *go_left])]
        for group, pair in zip(groups, passed, strict=True):
            i = table[group[0]][0] // layers
            pieces = halves(table, group)
            pair = [*pair, *(lax.ppermute(a, "dp", to_other) for a in pair)]
            body = functools.partial(far_kernel, n, layers, pieces)
            amount = 4 * sum(half for _, _, half, _ in pieces)
            (whole[i],) = placed(body, 4 * len(pieces), amount, w_tiles[i : i + 1], pair, whole[i])
        return (
            *(untiles(a, like.shape) for a, like in zip(whole, weights, strict=True)),
            *(untiles(a, like.shape) for a, like in zip(new_m, m, strict=True)),
            *(untiles(a, like.shape) for a, like in zip(new_v, v, strict=True)),
        )

    all_of, cut = P(None, None, None), P(None, "dp", None)
    return jax.shard_map(
        step,
        mesh=mesh,
        in_specs=(P(("rep", "dp"), None, None, None),) * 3 + (all_of,) * 3 + (cut,) * 6,
        out_specs=(P("rep", None, None),) * 3 + (P("rep", "dp", None),) * 6,
        check_vma=False,
    )
```
